32 devices in a mesh: gx: 8 (over y, x, core), gy: 4 (over z).
Axes of the slice: x: 2, y: 2, z: 4, core: 2. Of those that a mesh axis runs over, the one named last changes fastest.
Arguments:
- modes: bfloat16 [256, 128, 4, 3, 256], P('gx', 'gy'), may hold values from -6 to 6
- adv_index: int32 [8], replicated, may hold values from 0 to 255
Outputs:
- convection: float32 [256, 8, 256], P('gx', None, 'gy')
The draws below stay inside these ranges and needn't reach their ends.
All inputs are finite; a program needn't handle non-finite values.
Results may differ from the reference program's by a relative error of at most 0.0041.
Values may be sent and summed in bfloat16 or wider, within the bound.
A program may use at most 192 MiB of HBM per device.

```python
import math
import jax
import jax.numpy as jnp
from jax import lax

MODES = 256
ADV = 8
CX = 32
NX = 256
NY = 128
NZ = 4


def plant(result, key, smallest, high):
    spot = [jax.random.randint(jax.random.fold_in(key, axis), (), 0, length) for axis, length in enumerate(result.shape)]
    widest = result.shape.index(max(result.shape))
    neighbour = spot[:widest] + [(spot[widest] + 1) % result.shape[widest]] + spot[widest + 1:]
    return result.at[tuple(spot)].set(smallest).at[tuple(neighbour)].set(high)


def strengthened(result, stream_key, source, target, shards_of, factor):
    owner, partner = [(jnp.arange(result.shape[position]) // (result.shape[position] // shards_of)).reshape([-1 if axis == position else 1 for axis in range(result.ndim)]) for position in (source, target)]
    chosen = jax.random.permutation(stream_key, shards_of)[partner]
    strong = (owner == chosen) | (owner == (partner + shards_of // 2) % shards_of)
    return jnp.where(strong, factor * result, result)


def block_levels(key, dims, split, low, top_value):
    factor_of, own = 1.0, jax.random.fold_in(key, 6)
    for position, shards_of in split:
        draws = jnp.exp(jax.random.uniform(jax.random.fold_in(own, position), (shards_of,), jnp.float32, low / len(split), top_value / len(split)))
        factor_of = factor_of * jnp.repeat(draws, dims[position] // shards_of).reshape([-1 if axis == position else 1 for axis in range(len(dims))])
    return factor_of


def noise_with(own_key, extent, spread, most, split, heavy, held_as=jnp.bfloat16):
    array = spread * jax.random.normal(own_key, extent, jnp.float32)
    if split:
        array = array * block_levels(own_key, extent, split, -0.22, 0.18)
    return jnp.clip(strengthened(array, jax.random.fold_in(own_key, 3), *heavy), -most, most).astype(held_as)


def setup_inputs(seed: int = 0) -> dict:
    arg_keys = jax.random.split(jax.random.key(seed), 3)
    modes = noise_with(arg_keys[0], (NX, NY, NZ, 3, MODES), 1.0, 6.0, ((0, 8), (1, 4)), (0, 4, 8, 2.0))
    adv_index = plant(jax.random.randint(arg_keys[1], (ADV,), 0, MODES), jax.random.fold_in(arg_keys[1], 1), 0, MODES - 1).astype(jnp.int32)
    return dict(modes=modes, adv_index=adv_index)


def difference(padded, axis):
    length = padded.shape[axis] - 4

    def shifted(offset):
        return lax.slice_in_dim(padded, offset, offset + length, axis=axis).astype(jnp.float32)
    return (shifted(0) - shifted(4) + 8.0 * (shifted(3) - shifted(1))) / 12.0

def reference(modes, adv_index):
    widened = jnp.concatenate([modes[-2:], modes, modes[:2]], axis=0)
    widened = jnp.concatenate([widened[:, -2:], widened, widened[:, :2]], axis=1)
    widened = jnp.pad(widened, ((0, 0), (0, 0), (2, 2), (0, 0), (0, 0)))
    block_count = modes.shape[0] // CX

    def one_block(carry, which):
        start = (which * CX).astype(jnp.int32)
        slab = lax.dynamic_slice_in_dim(widened, start, CX + 4, 0)
        grad_x = difference(slab[:, 2:-2, 2:-2], 0).astype(jnp.bfloat16).astype(jnp.float32)
        grad_y = difference(slab[2:-2, :, 2:-2], 1).astype(jnp.bfloat16).astype(jnp.float32)
        grad_z = difference(slab[2:-2, 2:-2, :], 2).astype(jnp.bfloat16).astype(jnp.float32)
        center = slab[2:-2, 2:-2, 2:-2]
        advect = jnp.take(center, adv_index, axis=4).astype(jnp.float32)
        flat = center.reshape(-1, MODES)

        def one_mode(column):
            speed = lax.dynamic_index_in_dim(advect, column, 4, keepdims=False)
            field = speed[:, :, :, 0][..., None, None] * grad_x + speed[:, :, :, 1][..., None, None] * grad_y + speed[:, :, :, 2][..., None, None] * grad_z
            field = field.astype(jnp.bfloat16).reshape(-1, MODES)
            return lax.dot_general(flat, field, (((0,), (0,)), ((), ())), preferred_element_type=jnp.float32)
        pieces = lax.map(one_mode, jnp.arange(ADV, dtype=jnp.int32))
        return (carry + pieces, None)
    initial = jnp.zeros((ADV, MODES, MODES), jnp.float32)
    totals, _ = lax.scan(one_block, initial, jnp.arange(block_count, dtype=jnp.int32))
    factor = 1.0 / math.sqrt(3.0 * NX * NY * NZ)
    return jnp.transpose(totals, (1, 0, 2)) * factor
```

```python
import functools
import math

import jax
import jax.numpy as jnp
from jax import lax
from jax.experimental import pallas as pl
from jax.experimental.pallas import tpu as pltpu
from jax.sharding import PartitionSpec as P

PLANES = 2
LANES = 128


def stencil(back2, back1, ahead1, ahead2):
    return (back2 - ahead2 + 8.0 * (ahead1 - back1)) * (1.0 / 12.0)


def prepare(m_ref, pick_ref, turned_ref, speeds_ref, ahead_ref, flat):
    components, cells_z, cells_x, cells_y, width = m_ref.shape
    rows = PLANES * cells_z * cells_y

    def step(block, carry):
        for plane in range(PLANES):
            x = block * PLANES + plane
            for c in range(components):
                centre = [m_ref[c, z, x].astype(jnp.float32) for z in range(cells_z)]
                empty = jnp.zeros_like(centre[0])
                padded = [empty, empty] + centre + [empty, empty]
                for z in range(cells_z):
                    spot = pl.ds((plane * cells_z + z) * cells_y, cells_y)
                    value = stencil(padded[z], padded[z + 1], padded[z + 3], padded[z + 4])
                    ahead_ref[block, c, spot] = value.astype(jnp.bfloat16)
                    flat[c, spot] = m_ref[c, z, x]
        for c in range(components):
            speeds_ref[block, c] = jnp.dot(
                flat[c], pick_ref[...], preferred_element_type=jnp.float32
            ).astype(jnp.bfloat16)
            turned_ref[block, :, c * rows : (c + 1) * rows] = flat[c].T
        return carry

    lax.fori_loop(0, cells_x // PLANES, step, 0)


def kernel(advecting, m_ref, xb_ref, xa_ref, yh_ref, turned_ref, speeds_ref, ahead_ref, out_ref, slab, acc, grads):
    components, cells_z, cells_x, cells_y, width = m_ref.shape
    rows = PLANES * cells_z * cells_y
    tall = cells_y + yh_ref.shape[3]
    acc[...] = jnp.zeros_like(acc)
    slab[:, :, 0:2] = xb_ref[...]
    slab[:, :, cells_x + 2 : cells_x + 4] = xa_ref[...]

    def bring(x, carry):
        slab[:, :, x + 2] = m_ref[:, :, x]
        return carry

    lax.fori_loop(0, cells_x, bring, 0)

    def step(block, carry):
        for plane in range(PLANES):
            x = block * PLANES + plane
            for c in range(components):
                for z in range(cells_z):
                    spot = pl.ds((plane * cells_z + z) * cells_y, cells_y)

                    def along_x(offset):
                        return slab[c, z, x + 2 + offset].astype(jnp.float32)

                    rim = yh_ref[c, z, x].astype(jnp.float32)
                    column = jnp.concatenate([along_x(0), rim], axis=0)

                    def along_y(offset):
                        return pltpu.roll(column, (-offset) % tall, 0)[:cells_y]

                    for d, along in enumerate((along_x, along_y)):
                        value = stencil(along(-2), along(-1), along(1), along(2))
                        grads[d, c, spot] = value.astype(jnp.bfloat16)
        for j in range(advecting):
            speed = [
                jnp.broadcast_to(speeds_ref[block, d, :, j : j + 1].astype(jnp.float32), (rows, width))
                for d in range(3)
            ]
            fields = []
            for c in range(components):
                field = (
                    speed[0] * grads[0, c].astype(jnp.float32)
                    + speed[1] * grads[1, c].astype(jnp.float32)
                    + speed[2] * ahead_ref[block, c].astype(jnp.float32)
                )
                fields.append(field.astype(jnp.bfloat16))
            acc[j] += jnp.dot(
                turned_ref[block], jnp.concatenate(fields, axis=0), preferred_element_type=jnp.float32
            )
        return carry

    lax.fori_loop(0, cells_x // PLANES, step, 0)
    groups, high = out_ref.shape[0], out_ref.shape[1]
    for a in range(groups):
        for j in range(advecting):
            out_ref[a, :, j * width : (j + 1) * width] = acc[j, a * high : (a + 1) * high].astype(jnp.bfloat16)


def convect(inner, before, after, rim, pick, advecting, groups):
    components, cells_z, cells_x, cells_y, width = inner.shape
    rows = PLANES * cells_z * cells_y
    vmem = pl.BlockSpec(memory_space=pltpu.VMEM)
    blocks = cells_x // PLANES
    turned, speeds, ahead = pl.pallas_call(
        prepare,
        out_shape=[
            jax.ShapeDtypeStruct((blocks, width, components * rows), jnp.bfloat16),
            jax.ShapeDtypeStruct((blocks, 3, rows, LANES), jnp.bfloat16),
            jax.ShapeDtypeStruct((blocks, components, rows, width), jnp.bfloat16),
        ],
        in_specs=[vmem] * 2,
        out_specs=[vmem] * 3,
        scratch_shapes=[pltpu.VMEM((components, rows, width), jnp.bfloat16)],
        compiler_params=pltpu.CompilerParams(vmem_limit_bytes=28 * 1024 * 1024),
        cost_estimate=pl.CostEstimate(flops=20_000_000_000, bytes_accessed=30_000_000, transcendentals=0),
        name="prepare",
    )(inner, pick)
    return pl.pallas_call(
        functools.partial(kernel, advecting),
        out_shape=jax.ShapeDtypeStruct((groups, width // groups, advecting * width), jnp.bfloat16),
        in_specs=[vmem] * 7,
        out_specs=vmem,
        scratch_shapes=[
            pltpu.VMEM((components, cells_z, cells_x + 4, cells_y, width), jnp.bfloat16),
            pltpu.VMEM((advecting, width, width), jnp.float32),
            pltpu.VMEM((2, components, rows, width), jnp.bfloat16),
        ],
        compiler_params=pltpu.CompilerParams(vmem_limit_bytes=44 * 1024 * 1024),
        name="convect",
    )(inner, before, after, rim, turned, speeds, ahead)


def neighbours(cells, axis, dim):
    count = lax.axis_size(axis)
    head = lax.slice_in_dim(cells, 0, 2, axis=dim)
    tail = lax.slice_in_dim(cells, cells.shape[dim] - 2, cells.shape[dim], axis=dim)
    before = lax.ppermute(tail, axis, [(i, (i + 1) % count) for i in range(count)])
    after = lax.ppermute(head, axis, [((i + 1) % count, i) for i in range(count)])
    return before, after


def per_device(modes, adv_index):
    cells_x, cells_y, cells_z, components, width = modes.shape
    advecting = adv_index.shape[0]
    groups_x = lax.axis_size("gx")
    groups_y = lax.axis_size("gy")
    order = (3, 2, 0, 1, 4)
    before_x, after_x = neighbours(modes, "gx", 0)
    before_y, after_y = neighbours(modes, "gy", 1)
    gap = jnp.zeros((cells_x, 4, cells_z, components, width), modes.dtype)
    rim = jnp.concatenate([after_y, gap, before_y], axis=1)
    columns = jnp.pad(adv_index, (0, LANES - advecting), constant_values=-1)
    pick = (lax.broadcasted_iota(jnp.int32, (width, LANES), 0) == columns[None, :]).astype(jnp.bfloat16)
    partial = convect(
        jnp.transpose(modes, order),
        jnp.transpose(before_x, order),
        jnp.transpose(after_x, order),
        jnp.transpose(rim, order),
        pick,
        advecting,
        groups_x,
    )
    high, wide = width // groups_x, width // groups_y
    parts = lax.all_to_all(partial, "gx", 0, 0, tiled=True)
    owned = jnp.sum(parts.astype(jnp.float32), axis=0).astype(jnp.bfloat16)
    owned = jnp.transpose(owned.reshape(high, advecting, groups_y, wide), (2, 0, 1, 3))
    owned = lax.all_to_all(owned.reshape(groups_y, high, advecting * wide), "gy", 0, 0, tiled=True)
    total = jnp.sum(owned.astype(jnp.float32), axis=0)
    factor = 1.0 / math.sqrt(3.0 * cells_x * cells_y * cells_z * groups_x * groups_y)
    return total.reshape(high, advecting, wide) * factor


def solution(mesh):
    return jax.shard_map(
        per_device,
        mesh=mesh,
        in_specs=(P("gx", "gy", None, None, None), P()),
        out_specs=P("gx", None, "gy"),
        check_vma=False,
    )
```
